32 devices in a mesh: head: 2 (over x), outer: 4 (over y, core), inner: 4 (over z).
Axes of the slice: x: 2, y: 2, z: 4, core: 2. Of those that a mesh axis runs over, the one named last changes fastest.
Arguments:
- query_mant: bfloat16 [16, 1024, 128], P('outer', ('head', 'inner')), may hold values from -40 to 40
- key_mant: bfloat16 [1, 1024, 128], P(None, ('head', 'inner')), may hold values from -10 to 10
- value_mant: bfloat16 [1, 1024, 128], P(None, ('head', 'inner')), may hold values from -4 to 4
- out_grad: bfloat16 [16, 1024, 128], P('outer', ('head', 'inner')), may hold values from -4 to 4
- query_exp: int32 [16, 8], P('outer', ('head', 'inner')), may hold values from -1 to 1
- key_exp: int32 [1, 8], P(None, ('head', 'inner')), may hold values from -1 to 1
- value_exp: int32 [1, 8], P(None, ('head', 'inner')), may hold values from -1 to 1
- block_order: int32 [8], replicated, may hold values from 0 to 7, each once
Outputs:
- attended: bfloat16 [16, 1024, 128], P('outer', ('head', 'inner'))
- query_grad: bfloat16 [16, 1024, 128], P('outer', ('head', 'inner'))
- key_grad: bfloat16 [1, 1024, 128], P(None, ('head', 'inner'))
- value_grad: bfloat16 [1, 1024, 128], P(None, ('head', 'inner'))
The draws below stay inside these ranges and needn't reach their ends.
Inputs may be any that keep to these rules, and one draw needn't show every extreme that they name: `block_order`: every number of 0 to 7 once.
All inputs are finite; a program needn't handle non-finite values.
Results may differ from the reference program's by a relative error of at most 0.03.
Values may be sent and summed in bfloat16 or wider, within the bound.
A program may use at most 64 MiB of HBM per device.

```python
import math
import jax
import jax.numpy as jnp
from jax import lax

HD = 128
GROUP = 16
BLK = 128
HEADS = 16
KV_HEADS = 1
SEQ = 1024
NBLK = 8


def make_keys(key):
    base_keys = jnp.clip(jax.random.normal(jax.random.fold_in(key, 11), (KV_HEADS, SEQ, HD), jnp.float32), -4.0, 4.0)
    keys_all = base_keys
    return keys_all


def draw_key_mant(key, part):
    keys_all = make_keys(key)
    return keys_all.astype(jnp.bfloat16)


def draw_query_mant(key, part):
    drawn = jnp.clip(jax.random.normal(jax.random.fold_in(key, 21), (HEADS, SEQ, HD), jnp.float32), -4.0, 4.0)
    result = drawn
    return result.astype(jnp.bfloat16)


def with_ends(values, key, smallest, top_value):
    longest = values.shape.index(max(values.shape))
    spots = []
    for shift in (0, 1):
        where = [jax.random.randint(jax.random.fold_in(key, axis), (), 0, length) for axis, length in enumerate(values.shape)]
        where[longest] = (where[longest] + shift) % values.shape[longest]
        spots.append(tuple(where))
    return values.at[spots[0]].set(smallest).at[spots[1]].set(top_value)


def block_scale(own_key, extent, cuts, smallest, top_value):
    level, own = 1.0, jax.random.fold_in(own_key, 6)
    for axis_at, shards_of in cuts:
        draws = jnp.exp(jax.random.uniform(jax.random.fold_in(own, axis_at), (shards_of,), jnp.float32, smallest / len(cuts), top_value / len(cuts)))
        level = level * jnp.repeat(draws, extent[axis_at] // shards_of).reshape([-1 if axis == axis_at else 1 for axis in range(len(extent))])
    return level


def gaussian(rng, shape, spread, most, shards=(), held_as=jnp.bfloat16):
    values = jax.random.normal(rng, shape, jnp.float32) * spread
    if len(shards) > 0:
        values = block_scale(rng, shape, shards, -0.22, 0.18) * values
    return jnp.clip(values, min=-most, max=most).astype(held_as)


def setup_inputs(seed: int = 0) -> dict:
    keys = jax.random.split(jax.random.key(seed), 9)
    return {
        "query_mant": draw_query_mant(jax.random.fold_in(keys[8], 71), 0),
        "key_mant": draw_key_mant(jax.random.fold_in(keys[8], 71), 0),
        "value_mant": gaussian(keys[2], (KV_HEADS, SEQ, HD), 1.0, 4.0, ((1, 8),)),
        "out_grad": gaussian(keys[3], (HEADS, SEQ, HD), 1.0, 4.0, ((0, 4), (1, 8))),
        "query_exp": with_ends(jax.random.randint(keys[4], (HEADS, NBLK), -1, 2), jax.random.fold_in(keys[4], 1), -1, 1).astype(jnp.int32),
        "key_exp": with_ends(jax.random.randint(keys[5], (KV_HEADS, NBLK), -1, 2), jax.random.fold_in(keys[5], 1), -1, 1).astype(jnp.int32),
        "value_exp": with_ends(jax.random.randint(keys[6], (KV_HEADS, NBLK), -1, 2), jax.random.fold_in(keys[6], 1), -1, 1).astype(jnp.int32),
        "block_order": jax.random.permutation(keys[7], NBLK).astype(jnp.int32),
    }


def apply_scale(values_in, exps):
    factor = jnp.exp2(exps.astype(jnp.float32))
    factor = jnp.repeat(factor, BLK, axis=1)
    return (values_in.astype(jnp.float32) * factor[:, :, None]).astype(jnp.bfloat16)

def reference(query_mant, key_mant, value_mant, out_grad, query_exp, key_exp, value_exp, block_order):
    width = query_mant.shape[2]
    inv_root = 1.0 / math.sqrt(width)
    row_ids = jnp.arange(SEQ, dtype=jnp.int32)
    token_pos = block_order[row_ids // BLK] * BLK + row_ids % BLK
    visible = token_pos[None, :] <= token_pos[:, None]
    scaled_query = apply_scale(query_mant, query_exp)
    scaled_key = apply_scale(key_mant, key_exp)
    scaled_value = apply_scale(value_mant, value_exp)

    def one_head(index):
        group = (index // GROUP).astype(jnp.int32)
        head_q = lax.dynamic_index_in_dim(scaled_query, index, 0, keepdims=False)
        head_dout = lax.dynamic_index_in_dim(out_grad, index, 0, keepdims=False)
        head_k = lax.dynamic_index_in_dim(scaled_key, group, 0, keepdims=False)
        head_v = lax.dynamic_index_in_dim(scaled_value, group, 0, keepdims=False)
        scores = jnp.dot(head_q, head_k.T, preferred_element_type=jnp.float32) * inv_root
        scores = jnp.where(visible, scores, -1e+30)
        log_total = jax.nn.logsumexp(scores, axis=1)
        probs = jnp.where(visible, jnp.exp(scores - log_total[:, None]), 0.0)
        probs_low = probs.astype(jnp.bfloat16)
        attended = jnp.dot(probs_low, head_v, preferred_element_type=jnp.float32).astype(jnp.bfloat16)
        row_delta = lax.optimization_barrier(jnp.sum(head_dout.astype(jnp.float32) * attended.astype(jnp.float32), axis=1))
        dprob = jnp.dot(head_dout, head_v.T, preferred_element_type=jnp.float32)
        dscore = (probs * (dprob - row_delta[:, None])).astype(jnp.bfloat16)
        grad_q = jnp.dot(dscore, head_k, preferred_element_type=jnp.float32) * inv_root
        grad_k = jnp.dot(dscore.T, head_q, preferred_element_type=jnp.float32) * inv_root
        grad_v = jnp.dot(probs_low.T, head_dout, preferred_element_type=jnp.float32)
        return (attended, grad_q, grad_k, grad_v)
    attended, dq_all, dk_all, dv_all = lax.map(one_head, jnp.arange(HEADS, dtype=jnp.int32))
    q_fac = jnp.repeat(jnp.exp2(query_exp.astype(jnp.float32)), BLK, axis=1)[:, :, None]
    k_fac = jnp.repeat(jnp.exp2(key_exp.astype(jnp.float32)), BLK, axis=1)[:, :, None]
    v_fac = jnp.repeat(jnp.exp2(value_exp.astype(jnp.float32)), BLK, axis=1)[:, :, None]
    query_grad = (dq_all * q_fac).astype(jnp.bfloat16)
    dk_sum = lax.optimization_barrier(jnp.sum(dk_all.reshape(KV_HEADS, GROUP, SEQ, width), axis=1))
    dv_sum = lax.optimization_barrier(jnp.sum(dv_all.reshape(KV_HEADS, GROUP, SEQ, width), axis=1))
    key_grad = (dk_sum * k_fac).astype(jnp.bfloat16)
    value_grad = (dv_sum * v_fac).astype(jnp.bfloat16)
    return (attended, query_grad, key_grad, value_grad)
```

```python
import functools
import math

import jax
import jax.numpy as jnp
from jax import lax
from jax.experimental import pallas as pl
from jax.experimental.pallas import tpu as pltpu
from jax.sharding import PartitionSpec as P

GROUP = 16
BLK = 128
MESH = pl.DeviceIdType.MESH
F32 = jnp.float32
BF16 = jnp.bfloat16


def each(count, body):
    if count <= 8:
        for index in range(count):
            body(index)
    else:
        lax.fori_loop(0, count, lambda index, carry: (body(index), carry)[1], 0)


def power(exponent):
    return jnp.where(exponent > 0, 2.0, jnp.where(exponent < 0, 0.5, 1.0)).astype(F32)


def dot_nt(left, right):
    return lax.dot_general(left, right, (((1,), (1,)), ((), ())), preferred_element_type=F32)


def dot_tn(left, right):
    return lax.dot_general(left, right, (((0,), (0,)), ((), ())), preferred_element_type=F32)


def kernel(
    sizes,
    q_hbm,
    k_hbm,
    v_hbm,
    d_hbm,
    qe_hbm,
    ke_hbm,
    ve_hbm,
    order_hbm,
    o_ref,
    dq_ref,
    dk_ref,
    dv_ref,
    kv,
    right,
    scores,
    dprob,
    left,
    part,
    half,
    half_in,
    sums,
    sums_in,
    members,
    gather_send,
    gather_recv,
    pair_send,
    pair_recv,
    half_send,
    half_recv,
    sum_send,
    sum_recv,
    out_send,
    out_recv,
    q_ref,
    k_ref,
    v_ref,
    d_ref,
    qe_ref,
    ke_ref,
    ve_ref,
    order_ref,
    load_sem,
):
    heads_n, inner_n, outer_n = sizes
    loads = [
        pltpu.make_async_copy(source, target, load_sem.at[at])
        for at, (source, target) in enumerate(
            (
                (ke_hbm, ke_ref),
                (k_hbm, k_ref),
                (ve_hbm, ve_ref),
                (v_hbm, v_ref),
                (qe_hbm, qe_ref),
                (q_hbm, q_ref),
                (d_hbm, d_ref),
                (order_hbm, order_ref),
            )
        )
    ]
    heads, rows, width = q_ref.shape
    kv_count = k_ref.shape[0]
    count = heads_n * inner_n
    queries = heads * rows
    inv_root = 1.0 / math.sqrt(width)

    my_head = lax.axis_index("head")
    my_inner = lax.axis_index("inner")
    my_outer = lax.axis_index("outer")
    place = my_head * inner_n + my_inner
    core = lax.rem(my_outer, 2)
    mate = my_outer + 1 - 2 * core
    kv_index = my_outer * heads // GROUP

    offsets = [(a, b) for a in range(heads_n) for b in range(inner_n) if a or b]
    offsets.sort(key=lambda ab: min(ab[0], heads_n - ab[0]) + min(ab[1], inner_n - ab[1]))

    def ahead(off):
        return lax.rem(my_head + off[0], heads_n), lax.rem(my_inner + off[1], inner_n)

    def behind(off):
        return (
            lax.rem(my_head + heads_n - off[0], heads_n),
            lax.rem(my_inner + inner_n - off[1], inner_n),
        )

    def seq_id(pair):
        return {"head": pair[0], "inner": pair[1], "outer": my_outer}

    def outer_id(index):
        return {"head": my_head, "inner": my_inner, "outer": index}

    def index_of(pair):
        return pair[0] * inner_n + pair[1]

    barrier = pltpu.get_barrier_semaphore()
    for off in offsets:
        pl.semaphore_signal(barrier, inc=1, device_id=seq_id(ahead(off)), device_id_type=MESH)
    for step in range(1, outer_n):
        pl.semaphore_signal(
            barrier,
            inc=1,
            device_id=outer_id(lax.rem(my_outer + step, outer_n)),
            device_id_type=MESH,
        )
    for load in loads:
        load.start()
    for load in loads[:4]:
        load.wait()
    kv[0, place] = k_ref[kv_index] * power(ke_ref[kv_index]).astype(BF16)
    kv[1, place] = v_ref[kv_index] * power(ve_ref[kv_index]).astype(BF16)
    pl.semaphore_wait(barrier, len(offsets) + outer_n - 1)

    sends = []
    slots = {off: slot for slot, off in enumerate(offsets)}
    line = [off for off in offsets if off[0] == 0][::-1]
    across = [off for off in offsets if off[1] == 0]

    def pass_on(source, slot, device):
        return pltpu.make_async_remote_copy(
            src_ref=kv.at[core, source],
            dst_ref=kv.at[core, source],
            send_sem=gather_send.at[slot],
            recv_sem=gather_recv.at[slot],
            device_id=device,
            device_id_type=MESH,
        )

    gathers = {}
    direct = [off for off in offsets if off[0] and off[1] and min(off[1], inner_n - off[1]) == 1]
    for off in line + across + direct:
        copy = pass_on(place, slots[off], seq_id(ahead(off)))
        copy.start()
        gathers[off] = copy
        sends.append(copy)

    for load in loads[4:]:
        load.wait()
    for head in range(heads):
        right[0, head * rows : (head + 1) * rows] = q_ref[head] * power(qe_ref[head]).astype(BF16)
        right[1, head * rows : (head + 1) * rows] = d_ref[head]

    key_at = lax.broadcasted_iota(jnp.int32, (rows, queries), 0)
    row_at = lax.rem(lax.broadcasted_iota(jnp.int32, (rows, queries), 1), rows)
    lag = key_at - row_at
    own_order = order_ref[place]

    def score_block(index, top):
        reach = (own_order - order_ref[index]) * rows
        found = dot_nt(kv[0, index], right[0]) * (inv_root * math.log2(math.e))
        found = jnp.where(lag <= reach, found, -1e30)
        scores[index] = found
        dprob[index] = dot_nt(kv[1, index], right[1])
        return jnp.maximum(top, jnp.max(found.reshape(rows // 8, 8, queries), axis=0))

    top = score_block(place, jnp.full((8, queries), -1e30, F32))
    arrivals = across + line + [(a, b) for _, b in line for a, _ in across]
    waiting = None
    for off in arrivals:
        gathers[off].wait_recv()
        source = index_of(behind(off))
        if off[0] == 0:
            for step, _ in across:
                to = (step, off[1])
                if to in direct:
                    continue
                device = seq_id((lax.rem(my_head + step, heads_n), my_inner))
                copy = pass_on(source, slots[to], device)
                copy.start()
                gathers[to] = copy
                sends.append(copy)
        copy = pltpu.make_async_remote_copy(
            src_ref=kv.at[core, source],
            dst_ref=kv.at[core, source],
            send_sem=pair_send.at[slots[off]],
            recv_sem=pair_recv.at[slots[off]],
            device_id=outer_id(mate),
            device_id_type=MESH,
        )
        copy.start()
        sends.append(copy)
        if waiting is not None:
            waiting[0].wait_recv()
            top = score_block(waiting[1], top)
        waiting = (copy, source)
    if waiting is not None:
        waiting[0].wait_recv()
        top = score_block(waiting[1], top)

    best = jnp.max(top, axis=0, keepdims=True)
    half_in_f32 = jnp.zeros((8, queries), F32)

    def weigh(index, carry):
        total, cross = carry
        weight = jnp.exp2(scores[index] - best)
        scores[index] = weight
        total = total + jnp.sum(weight.reshape(rows // 8, 8, queries), axis=0)
        cross = cross + jnp.sum((weight * dprob[index]).reshape(rows // 8, 8, queries), axis=0)
        return total, cross

    carry = (half_in_f32, half_in_f32)
    if count <= 8:
        for index in range(count):
            carry = weigh(index, carry)
    else:
        carry = lax.fori_loop(0, count, weigh, carry)
    inverse = 1.0 / jnp.sum(carry[0], axis=0, keepdims=True)
    delta = jnp.sum(carry[1], axis=0, keepdims=True) * inverse

    def finish(index):
        prob = scores[index] * inverse
        left[1, index] = prob.astype(BF16)
        left[0, index] = (prob * (dprob[index] - delta)).astype(BF16)

    given = 1 - core

    def pair_copy(index):
        return pltpu.make_async_remote_copy(
            src_ref=half.at[index],
            dst_ref=half_in.at[index],
            send_sem=half_send.at[index],
            recv_sem=half_recv.at[index],
            device_id=outer_id(mate),
            device_id_type=MESH,
        )

    far = [(slot, off) for slot, off in enumerate(offsets)][::-1]
    targets = [index_of(ahead(off)) for _, off in far]
    for target in targets + [place]:
        finish(target)
        half[target] = jnp.dot(
            left[given, target], right[given], preferred_element_type=F32
        ).astype(BF16)
        pair_copy(target).start()

    sum_copies = []
    for (slot, off), target in zip(far, targets):
        kept = jnp.dot(left[core, target], right[core], preferred_element_type=F32)
        pair_copy(target).wait_recv()
        sums[slot] = (kept + half_in[target].astype(F32)).astype(BF16)
        copy = pltpu.make_async_remote_copy(
            src_ref=sums.at[slot],
            dst_ref=sums_in.at[slot],
            send_sem=sum_send.at[slot],
            recv_sem=sum_recv.at[slot],
            device_id=seq_id(ahead(off)),
            device_id_type=MESH,
        )
        copy.start()
        sum_copies.append((slot, copy))
        sends.append(copy)
    kept = jnp.dot(left[core, place], right[core], preferred_element_type=F32)
    pair_copy(place).wait_recv()
    part[...] = kept + half_in[place].astype(F32)

    flat = count * rows
    out_t = dot_tn(kv[1].reshape(flat, width), left[1].reshape(flat, queries))
    for head in range(heads):
        o_ref[head] = out_t[:, head * rows : (head + 1) * rows].T.astype(BF16)
    dq_t = dot_tn(kv[0].reshape(flat, width), left[0].reshape(flat, queries))
    for head in range(heads):
        scale = power(qe_ref[head]) * inv_root
        dq_ref[head] = (dq_t[:, head * rows : (head + 1) * rows] * scale).T.astype(BF16)

    total = part[...]
    for slot, copy in sum_copies:
        copy.wait_recv()
        total = total + sums_in[slot].astype(F32)
    members[my_outer] = total.astype(BF16)

    out_copies = []
    for step in range(1, outer_n):
        copy = pltpu.make_async_remote_copy(
            src_ref=members.at[my_outer],
            dst_ref=members.at[my_outer],
            send_sem=out_send.at[step - 1],
            recv_sem=out_recv.at[step - 1],
            device_id=outer_id(lax.rem(my_outer + step, outer_n)),
            device_id_type=MESH,
        )
        copy.start()
        out_copies.append(copy)
        sends.append(copy)
    for copy in out_copies:
        copy.wait_recv()
    span = outer_n // kv_count
    for group in range(kv_count):
        key_sum = jnp.zeros((rows, width), F32)
        value_sum = jnp.zeros((rows, width), F32)
        for member in range(group * span, (group + 1) * span, 2):
            key_sum = key_sum + members[member].astype(F32)
            value_sum = value_sum + members[member + 1].astype(F32)
        dk_ref[group] = (key_sum * (power(ke_ref[group]) * inv_root)).astype(BF16)
        dv_ref[group] = (value_sum * power(ve_ref[group])).astype(BF16)

    for copy in sends:
        copy.wait_send()
    each(count, lambda index: pair_copy(index).wait_send())


def store_kernel(*refs):
    stores = [
        pltpu.make_async_copy(refs[at], refs[4 + at], refs[8].at[at]) for at in range(4)
    ]
    for store in stores:
        store.start()
    for store in stores:
        store.wait()


def on_device(
    query_mant, key_mant, value_mant, out_grad, query_exp, key_exp, value_exp, block_order, sizes
):
    heads, rows, width = query_mant.shape
    kv_count = key_mant.shape[0]
    heads_n, inner_n, outer_n = sizes
    count = heads_n * inner_n
    queries = heads * rows
    assert rows == BLK and outer_n % (2 * kv_count) == 0 and heads * outer_n == GROUP * kv_count
    dma = pltpu.SemaphoreType.DMA
    peers = max(count - 1, 1)
    hbm = pl.BlockSpec(memory_space=pltpu.HBM)
    vmem = pl.BlockSpec(memory_space=pltpu.VMEM)
    results = pl.pallas_call(
        functools.partial(kernel, sizes),
        out_shape=(
            pltpu.VMEM(query_mant.shape, BF16),
            pltpu.VMEM(query_mant.shape, BF16),
            pltpu.VMEM(key_mant.shape, BF16),
            pltpu.VMEM(key_mant.shape, BF16),
        ),
        in_specs=[hbm] * 8,
        out_specs=(vmem,) * 4,
        scratch_shapes=[
            pltpu.VMEM((2, count, rows, width), BF16),
            pltpu.VMEM((2, queries, width), BF16),
            pltpu.VMEM((count, rows, queries), F32),
            pltpu.VMEM((count, rows, queries), F32),
            pltpu.VMEM((2, count, rows, queries), BF16),
            pltpu.VMEM((rows, width), F32),
            pltpu.VMEM((count, rows, width), BF16),
            pltpu.VMEM((count, rows, width), BF16),
            pltpu.VMEM((peers, rows, width), BF16),
            pltpu.VMEM((peers, rows, width), BF16),
            pltpu.VMEM((outer_n, rows, width), BF16),
            dma((peers,)),
            dma((peers,)),
            dma((peers,)),
            dma((peers,)),
            dma((count,)),
            dma((count,)),
            dma((peers,)),
            dma((peers,)),
            dma((outer_n,)),
            dma((outer_n,)),
            pltpu.VMEM(query_mant.shape, BF16),
            pltpu.VMEM(key_mant.shape, BF16),
            pltpu.VMEM(key_mant.shape, BF16),
            pltpu.VMEM(query_mant.shape, BF16),
            pltpu.SMEM((heads,), jnp.int32),
            pltpu.SMEM((kv_count,), jnp.int32),
            pltpu.SMEM((kv_count,), jnp.int32),
            pltpu.SMEM(block_order.shape, jnp.int32),
            dma((8,)),
        ],
        compiler_params=pltpu.CompilerParams(
            collective_id=0, has_side_effects=True
        ),
    )(
        query_mant,
        key_mant,
        value_mant,
        out_grad,
        query_exp.reshape(-1),
        key_exp.reshape(-1),
        value_exp.reshape(-1),
        block_order,
    )
    return pl.pallas_call(
        store_kernel,
        out_shape=tuple(jax.ShapeDtypeStruct(found.shape, found.dtype) for found in results),
        in_specs=[vmem] * 4,
        out_specs=(hbm,) * 4,
        scratch_shapes=[dma((4,))],
    )(*(pltpu.with_memory_space_constraint(found, pltpu.VMEM) for found in results))


def solution(mesh):
    sizes = (mesh.shape["head"], mesh.shape["inner"], mesh.shape["outer"])
    placed = (
        P("outer", ("head", "inner"), None),
        P(None, ("head", "inner"), None),
        P(None, ("head", "inner"), None),
        P("outer", ("head", "inner"), None),
        P("outer", ("head", "inner")),
        P(None, ("head", "inner")),
        P(None, ("head", "inner")),
        P(),
    )
    return jax.shard_map(
        functools.partial(on_device, sizes=sizes),
        mesh=mesh,
        in_specs=placed,
        out_specs=(
            P("outer", ("head", "inner"), None),
            P("outer", ("head", "inner"), None),
            P(None, ("head", "inner"), None),
            P(None, ("head", "inner"), None),
        ),
        check_vma=False,
    )
```
